32 devices in a mesh: panel: 8 (over y, x, core), samp: 4 (over z).
Axes of the slice: x: 2, y: 2, z: 4, core: 2. Of those that a mesh axis runs over, the one named last changes fastest.
Arguments:
- called_allele_tallies: int32 [2048, 1024], P('samp'), may hold values from 0 to 2
- presence_flags: int32 [2048, 1024], P('samp'), may hold values 0 or 1
- reference_panel_strands: int32 [16384, 1024], P('panel'), may hold values from 0 to 1
- softmax_sharpness: float32 [2048], P('samp'), may hold values from 0.02 to 4
- trait_measurements: float32 [2048], P('samp'), may hold values from -8 to 8
- cohort_membership: int32 [2048], P('samp'), may hold values from 0 to 7, as said below
Outputs:
- dosage_out: bfloat16 [2048, 1024], P('samp', 'panel')
- zscore: float32 [1024], P('panel')
The draws below stay inside these ranges and needn't reach their ends.
Inputs may be any that keep to these rules, and one draw needn't show every extreme that they name: `cohort_membership`: every group id from 0 to 7 occurs.
All inputs are finite; a program needn't handle non-finite values. No bound on the sum of `presence_flags` on one device may be relied on, other than what follows from the above.
Results may differ from the reference program's by a relative error of at most 0.0055.
Values sent between devices are 32-bit elements; how exact they have to be, the bound alone decides.
A program may use at most 64 MiB of HBM per device.

```python
import jax
import jax.numpy as jnp
from jax import lax

SPAN_MARKERS = 1024
GROUPS = 8
HAPLOTYPES = 16384
SAMPLES = 2048


def draw_reference_panel_strands(key, part):
    key_base = jax.random.fold_in(key, 11)
    key_noise = jax.random.fold_in(key, 12)
    base_level = jax.random.randint(key_base, (SPAN_MARKERS,), 100, 700)
    noise = jax.random.randint(key_noise, (HAPLOTYPES, SPAN_MARKERS), 0, 1000)
    rows = jnp.arange(HAPLOTYPES, dtype=jnp.int32)[:, None]
    bound = base_level[None, :] * (HAPLOTYPES + 2 * rows) // (3 * HAPLOTYPES)
    return (noise < bound).astype(jnp.int32)


def draw_softmax_sharpness(key, part):
    uniform_draw = jax.random.uniform(jax.random.fold_in(key, 21), (SAMPLES,), jnp.float32)
    values = jnp.exp(jnp.log(0.02) + uniform_draw * jnp.log(15.0))
    return values.astype(jnp.float32)


def draw_trait_measurements(key, part):
    rows = jnp.arange(SAMPLES, dtype=jnp.float32)
    ramp = 0.5 + 1.5 * rows / SAMPLES
    noise = jax.random.normal(jax.random.fold_in(key, 32), (SAMPLES,), jnp.float32)
    values = ramp * noise
    return jnp.clip(values, -8.0, 8.0).astype(jnp.float32)


def draw_cohort_membership(key, part):
    drawn = jax.random.randint(jax.random.fold_in(key, 41), (SAMPLES,), 0, GROUPS)
    rows = jnp.arange(SAMPLES, dtype=jnp.int32)
    return jnp.where(rows < GROUPS, rows, drawn).astype(jnp.int32)


def set_ends(values, stream_key, smallest, high):
    extent = values.shape
    index_at = [jax.random.randint(jax.random.fold_in(stream_key, axis), (), 0, extent[axis]) for axis in range(len(extent))]
    values = values.at[tuple(index_at)].set(smallest)
    longest = extent.index(max(extent))
    index_at[longest] = (index_at[longest] + 1) % extent[longest]
    return values.at[tuple(index_at)].set(high)


def setup_inputs(seed: int = 0) -> dict:
    splits = jax.random.split(jax.random.key(seed), 7)
    return {
        "called_allele_tallies": set_ends(jax.random.randint(splits[0], (SAMPLES, SPAN_MARKERS), 0, 3), jax.random.fold_in(splits[0], 1), 0, 2).astype(jnp.int32),
        "presence_flags": set_ends((jax.random.randint(splits[1], (SAMPLES, SPAN_MARKERS), 0, 4) < 3).astype(jnp.int32), jax.random.fold_in(splits[1], 1), 0, 1),
        "reference_panel_strands": draw_reference_panel_strands(jax.random.fold_in(splits[6], 71), 0),
        "softmax_sharpness": draw_softmax_sharpness(jax.random.fold_in(splits[6], 71), 0),
        "trait_measurements": draw_trait_measurements(jax.random.fold_in(splits[6], 71), 0),
        "cohort_membership": draw_cohort_membership(jax.random.fold_in(splits[6], 71), 0),
    }


log_two = 0.6931471805599453

def reference(called_allele_tallies, presence_flags, reference_panel_strands, softmax_sharpness, trait_measurements, cohort_membership):
    hap_float = reference_panel_strands.astype(jnp.float32)
    allele_freq = lax.optimization_barrier(jnp.sum(hap_float, axis=0)) / HAPLOTYPES
    geno_float = called_allele_tallies.astype(jnp.float32)
    observed_f = presence_flags.astype(jnp.float32)
    demeaned_expected_count = (observed_f * (geno_float - 2.0 * allele_freq[None, :])).astype(jnp.bfloat16)
    tile_first_entry = lax.optimization_barrier(jnp.sum(demeaned_expected_count.astype(jnp.float32) * allele_freq[None, :], axis=1))
    hap_bf = reference_panel_strands.astype(jnp.bfloat16)
    entries_in_tile = min(SAMPLES, 512)
    tile_ordinal = SAMPLES // entries_in_tile

    def whole_matrix_tile(pieces):
        cen, offset, heat = pieces
        raw_efficient_statistic = lax.dot_general(cen, hap_bf, (((1,), (1,)), ((), ())), preferred_element_type=jnp.float32)
        panel_match_energies = heat[:, None] * (raw_efficient_statistic - offset[:, None])
        peak_steps = jnp.ceil(lax.optimization_barrier(jnp.max(panel_match_energies, axis=1)) / log_two)
        weights = jnp.exp(panel_match_energies - log_two * peak_steps[:, None])
        weight_total = lax.optimization_barrier(jnp.sum(weights, axis=1))
        summed = jnp.dot(weights.astype(jnp.bfloat16), hap_bf, preferred_element_type=jnp.float32)
        return 2.0 * summed / weight_total[:, None]
    expected_allele_count = lax.map(whole_matrix_tile, (demeaned_expected_count.reshape(tile_ordinal, entries_in_tile, SPAN_MARKERS), tile_first_entry.reshape(tile_ordinal, entries_in_tile), softmax_sharpness.reshape(tile_ordinal, entries_in_tile)))
    expected_allele_count = expected_allele_count.reshape(SAMPLES, SPAN_MARKERS)
    dosage = jnp.where(presence_flags == 1, geno_float, expected_allele_count)
    dosage_out = dosage.astype(jnp.bfloat16)
    member = (cohort_membership[:, None] == jnp.arange(GROUPS, dtype=jnp.int32)[None, :]).astype(jnp.float32)
    group_sum = jnp.dot(trait_measurements, member, precision=lax.Precision.HIGHEST)
    group_count = lax.optimization_barrier(jnp.sum(member, axis=0))
    group_mean = group_sum / group_count
    resid = trait_measurements - jnp.dot(member, group_mean, precision=lax.Precision.HIGHEST)
    sigma = jnp.sum(resid * resid) / (SAMPLES - GROUPS)
    score_u = jnp.dot(resid, dosage, precision=lax.Precision.HIGHEST)
    dose_mean = lax.optimization_barrier(jnp.sum(dosage, axis=0)) / SAMPLES
    spread = lax.optimization_barrier(jnp.sum(dosage * dosage, axis=0)) / SAMPLES - dose_mean * dose_mean
    zscore = score_u / jnp.sqrt(sigma * SAMPLES * (spread + 1e-05))
    return (dosage_out, zscore)
```

```python
import functools

import jax
import jax.numpy as jnp
from jax import lax
from jax.experimental import pallas as pl
from jax.experimental.pallas import tpu as pltpu
from jax.sharding import PartitionSpec as P

GROUPS = 8


log_two = 0.6931471805599453


def on_device(
    called_allele_tallies,
    presence_flags,
    reference_panel_strands,
    softmax_sharpness,
    trait_measurements,
    cohort_membership,
):
    panel_count = lax.axis_size("panel")
    sample_rows, variants = called_allele_tallies.shape
    local_haps = reference_panel_strands.shape[0]
    hap_float = reference_panel_strands.astype(jnp.float32)
    allele_counts = lax.psum(jnp.sum(hap_float, axis=0), "panel")
    allele_freq = allele_counts / float(local_haps * panel_count)
    geno_float = called_allele_tallies.astype(jnp.float32)
    observed_f = presence_flags.astype(jnp.float32)
    demeaned_expected_count = (observed_f * (geno_float - 2.0 * allele_freq[None, :])).astype(
        jnp.bfloat16
    )
    tile_first_entry = jnp.sum(
        demeaned_expected_count.astype(jnp.float32) * allele_freq[None, :], axis=1
    )
    hap_bf = reference_panel_strands.astype(jnp.bfloat16)
    raw_efficient_statistic = lax.dot_general(
        demeaned_expected_count,
        hap_bf,
        (((1,), (1,)), ((), ())),
        preferred_element_type=jnp.float32,
    )
    panel_match_energies = softmax_sharpness[:, None] * (
        raw_efficient_statistic - tile_first_entry[:, None]
    )
    local_steps = jnp.ceil(jnp.max(panel_match_energies, axis=1) / log_two)
    share = variants // panel_count
    first_column = lax.axis_index("panel") * share
    peak_steps = lax.pmax(local_steps, "panel")
    weights = jnp.exp(panel_match_energies - log_two * peak_steps[:, None])
    weight_total = lax.psum(jnp.sum(weights, axis=1), "panel")
    partial_dose = 2.0 * jnp.dot(
        weights.astype(jnp.bfloat16), hap_bf, preferred_element_type=jnp.float32
    )
    own_dose = lax.psum_scatter(partial_dose, "panel", scatter_dimension=1, tiled=True)
    expected_allele_count = own_dose / weight_total[:, None]
    own_geno = lax.dynamic_slice_in_dim(geno_float, first_column, share, 1)
    own_observed = lax.dynamic_slice_in_dim(presence_flags, first_column, share, 1)
    dosage = jnp.where(own_observed == 1, own_geno, expected_allele_count)
    dosage_out = dosage.astype(jnp.bfloat16)
    member = (cohort_membership[:, None] == jnp.arange(GROUPS, dtype=jnp.int32)[None, :]).astype(
        jnp.float32
    )
    group_sum_local = jnp.dot(trait_measurements, member, precision=lax.Precision.HIGHEST)
    group_count_local = jnp.sum(member, axis=0)
    dose_sum_local = jnp.sum(dosage, axis=0)
    dose_square_local = jnp.sum(dosage * dosage, axis=0)
    all_samples = float(sample_rows * lax.axis_size("samp"))
    group_sum, group_count = lax.psum((group_sum_local, group_count_local), "samp")
    group_mean = group_sum / group_count
    resid = trait_measurements - jnp.dot(member, group_mean, precision=lax.Precision.HIGHEST)
    local_score = jnp.dot(resid, dosage, precision=lax.Precision.HIGHEST)
    score_u, dose_sum, dose_square, resid_square = lax.psum(
        (local_score, dose_sum_local, dose_square_local, jnp.sum(resid * resid)), "samp"
    )
    sigma = resid_square / (all_samples - GROUPS)
    dose_mean = dose_sum / all_samples
    spread = dose_square / all_samples - dose_mean * dose_mean
    zscore = score_u / jnp.sqrt(sigma * all_samples * (spread + 1e-05))
    return (dosage_out, zscore)


MESH = pl.DeviceIdType.MESH
LANES = 128
HAP_TILE = 256
ROWS = 32
VMEM_BYTES = 60 * 1024 * 1024


def lane_copies(row):
    blocks = [
        jnp.broadcast_to(row[:, k : k + LANES], (LANES, LANES)).T
        for k in range(0, row.shape[1], LANES)
    ]
    return jnp.concatenate(blocks, axis=0)


def as_row(column):
    blocks = [
        jnp.broadcast_to(column[k : k + LANES], (LANES, LANES)).T[0:1]
        for k in range(0, column.shape[0], LANES)
    ]
    return jnp.concatenate(blocks, axis=1)


def fused(
    panel_count,
    samp_count,
    tallies_hbm,
    flags_hbm,
    strands_hbm,
    sharp_ref,
    trait_ref,
    cohort_ref,
    dosage_ref,
    zscore_ref,
    strands_ref,
    hap_ref,
    tallies_ref,
    flags_ref,
    centred_ref,
    logits_ref,
    weights_ref,
    counts_ref,
    peaks_ref,
    totals_ref,
    groups_ref,
    stats_ref,
    sharp_col,
    offset_col,
    steps_col,
    run_ref,
    part_ref,
    sib_ref,
    out_ref,
    in_ref,
    strand_sems,
    load_sems,
    count_send,
    count_recv,
    peak_send,
    peak_recv,
    total_send,
    total_recv,
    group_send,
    group_recv,
    stat_send,
    stat_recv,
    sib_send,
    sib_recv,
    hop_send,
    hop_recv,
):
    me = lax.axis_index("panel")
    depth = lax.axis_index("samp")
    samples, variants = tallies_ref.shape
    haps = strands_ref.shape[0]
    pieces = haps // HAP_TILE
    core = me % 2
    x = (me // 2) % 2
    y = me // 4
    sibling = me + 1 - 2 * core
    x_peer = me + 2 - 4 * x
    y_peer = me + 4 - 8 * y
    first_peer = x_peer + core * (y_peer - x_peer)
    second_peer = y_peer + core * (x_peer - y_peer)

    def strand_load(i):
        rows = pl.ds(i * HAP_TILE, HAP_TILE)
        return pltpu.make_async_copy(
            strands_hbm.at[rows], strands_ref.at[rows], strand_sems.at[i]
        )

    for i in range(pieces):
        strand_load(i).start()
    flag_load = pltpu.make_async_copy(flags_hbm, flags_ref, load_sems.at[0])
    tally_load = pltpu.make_async_copy(tallies_hbm, tallies_ref, load_sems.at[1])
    flag_load.start()
    tally_load.start()

    barrier = pltpu.get_barrier_semaphore()
    for d in range(1, panel_count):
        pl.semaphore_signal(
            barrier, inc=1, device_id={"panel": (me + d) % panel_count}, device_id_type=MESH
        )
    for d in range(1, samp_count):
        pl.semaphore_signal(
            barrier, inc=1, device_id={"samp": (depth + d) % samp_count}, device_id_type=MESH
        )
    pl.semaphore_wait(barrier, panel_count + samp_count - 2)

    def share_out(ref, send, recv, axis, count, mine):
        copies = []
        for d in range(1, count):
            copy = pltpu.make_async_remote_copy(
                src_ref=ref.at[mine],
                dst_ref=ref.at[mine],
                send_sem=send.at[d - 1],
                recv_sem=recv.at[d - 1],
                device_id={axis: (mine + d) % count},
                device_id_type=MESH,
            )
            copy.start()
            copies.append(copy)

        def arrive():
            for d in range(1, count):
                slot = (mine + count - d) % count
                pltpu.make_async_remote_copy(
                    src_ref=ref.at[slot],
                    dst_ref=ref.at[slot],
                    send_sem=send.at[d - 1],
                    recv_sem=recv.at[d - 1],
                    device_id={axis: (mine + d) % count},
                    device_id_type=MESH,
                ).wait_recv()

        def sent():
            for copy in copies:
                copy.wait_send()

        return arrive, sent

    trait = trait_ref[...]
    member = (
        lax.broadcasted_iota(jnp.int32, (GROUPS, samples), 0)
        == jnp.broadcast_to(cohort_ref[...], (GROUPS, samples))
    ).astype(jnp.float32)
    group_sum = jnp.sum(member * trait, axis=1, keepdims=True)
    group_count = jnp.sum(member, axis=1, keepdims=True)
    lane = lax.broadcasted_iota(jnp.int32, (GROUPS, LANES), 1)
    groups_ref[depth] = jnp.where(lane == 0, group_sum, group_count)
    groups_arrive, groups_sent = share_out(
        groups_ref, group_send, group_recv, "samp", samp_count, depth
    )
    sharp_col[...] = lane_copies(sharp_ref[...])

    def convert_piece(i, acc):
        strand_load(i).wait()

        def convert_rows(r, acc):
            start = pl.multiple_of(i * HAP_TILE + r * ROWS, ROWS)
            strands = strands_ref[pl.ds(start, ROWS)]
            hap_ref[pl.ds(start, ROWS)] = strands.astype(jnp.float32).astype(jnp.bfloat16)
            for k in range(0, ROWS, 8):
                acc = acc + strands[k : k + 8]
            return acc

        return lax.fori_loop(0, HAP_TILE // ROWS, convert_rows, acc)

    acc = lax.fori_loop(0, pieces, convert_piece, jnp.zeros((8, variants), jnp.int32))
    counts_ref[me] = jnp.sum(acc.astype(jnp.float32), axis=0, keepdims=True)
    counts_arrive, counts_sent = share_out(
        counts_ref, count_send, count_recv, "panel", panel_count, me
    )
    flag_load.wait()
    tally_load.wait()

    groups_arrive()
    group_all = groups_ref[0]
    for k in range(1, samp_count):
        group_all = group_all + groups_ref[k]
    group_mean = group_all[:, 0:1] / group_all[:, 1:2]
    resid = trait - jnp.sum(member * group_mean, axis=0, keepdims=True)
    resid_square = jnp.sum(resid * resid, axis=1, keepdims=True)

    counts_arrive()
    counts = counts_ref[0]
    for k in range(1, panel_count):
        counts = counts + counts_ref[k]
    freq = counts / float(haps * panel_count)

    def centre(r, _):
        rows = pl.ds(pl.multiple_of(r * ROWS, ROWS), ROWS)
        seen = flags_ref[rows].astype(jnp.float32)
        geno = tallies_ref[rows].astype(jnp.float32)
        centred = (seen * (geno - 2.0 * freq)).astype(jnp.bfloat16)
        centred_ref[rows] = centred
        offset = jnp.sum(centred.astype(jnp.float32) * freq, axis=1, keepdims=True)
        offset_col[rows] = jnp.broadcast_to(offset, (ROWS, LANES))
        return 0

    lax.fori_loop(0, samples // ROWS, centre, 0)

    run_ref[...] = jnp.full_like(run_ref, -jnp.inf)

    def match(i, _):
        hap = hap_ref[pl.ds(pl.multiple_of(i * HAP_TILE, HAP_TILE), HAP_TILE)]
        raw = lax.dot_general(
            centred_ref[...], hap, (((1,), (1,)), ((), ())), preferred_element_type=jnp.float32
        )
        sharp = sharp_col[...]
        offset = offset_col[...]
        best = run_ref[...]
        for k in range(0, HAP_TILE, LANES):
            energy = sharp * (raw[:, k : k + LANES] - offset)
            logits_ref[i, :, k : k + LANES] = energy
            best = jnp.maximum(best, energy)
        run_ref[...] = best
        return 0

    lax.fori_loop(0, pieces, match, 0)
    steps = jnp.ceil(jnp.max(run_ref[...], axis=1, keepdims=True) / log_two)
    steps_col[...] = jnp.broadcast_to(steps, steps_col.shape)
    local_steps = as_row(steps)
    peaks_ref[me] = local_steps
    peaks_arrive, peaks_sent = share_out(peaks_ref, peak_send, peak_recv, "panel", panel_count, me)

    run_ref[...] = jnp.zeros_like(run_ref)

    def weigh(r, _):
        rows = pl.ds(pl.multiple_of(r * ROWS, ROWS), ROWS)
        shift = log_two * steps_col[rows]
        total = jnp.zeros((ROWS, LANES), jnp.float32)
        for i in range(pieces):
            for k in range(0, HAP_TILE, LANES):
                weight = jnp.exp(logits_ref[i, rows, k : k + LANES] - shift)
                total = total + weight
                first = i * HAP_TILE + k
                weights_ref[rows, first : first + LANES] = weight.astype(jnp.bfloat16)
        run_ref[rows] = total
        return 0

    lax.fori_loop(0, samples // ROWS, weigh, 0)
    totals_ref[me] = as_row(jnp.sum(run_ref[...], axis=1, keepdims=True))
    totals_arrive, totals_sent = share_out(
        totals_ref, total_send, total_recv, "panel", panel_count, me
    )

    def allele_sums(chip):
        columns = pl.ds(pl.multiple_of(chip * 2 * LANES, 2 * LANES), 2 * LANES)
        return jnp.dot(
            weights_ref[...], hap_ref[:, columns], preferred_element_type=jnp.float32
        )

    def hand_over(i):
        copy = pltpu.make_async_remote_copy(
            src_ref=part_ref.at[i, 1 - core],
            dst_ref=sib_ref.at[i],
            send_sem=sib_send.at[i],
            recv_sem=sib_recv.at[i],
            device_id={"panel": sibling},
            device_id_type=MESH,
        )
        copy.start()
        return copy

    def hop(i, peer):
        copy = pltpu.make_async_remote_copy(
            src_ref=out_ref.at[i],
            dst_ref=in_ref.at[i],
            send_sem=hop_send.at[i],
            recv_sem=hop_recv.at[i],
            device_id={"panel": peer},
            device_id_type=MESH,
        )
        copy.start()
        return copy

    diag_chip = (1 - y) * 2 + 1 - x
    x_chip = y * 2 + 1 - x
    y_chip = (1 - y) * 2 + x
    own_chip = y * 2 + x
    handed = []
    scale = None
    hops = []
    for i, chip in enumerate((diag_chip, x_chip, y_chip, own_chip)):
        part = allele_sums(chip)
        if i == 0:
            peaks_arrive()
            top = peaks_ref[0]
            for k in range(1, panel_count):
                top = jnp.maximum(top, peaks_ref[k])
            steps_col[...] = lane_copies(jnp.exp2(local_steps - top))
        scale = steps_col[...]
        part_ref[i, 0] = scale * part[:, :LANES]
        part_ref[i, 1] = scale * part[:, LANES:]
        handed.append(hand_over(i))
        if i == 1:
            handed[0].wait_recv()
            out_ref[0] = part_ref[0, core] + sib_ref[0]
            hops.append(hop(0, first_peer))

    near = 1 + core
    far = 2 - core
    handed[1].wait_recv()
    handed[2].wait_recv()
    out_ref[1] = part_ref[near, core] + sib_ref[near]
    hops.append(hop(1, first_peer))
    out_ref[2] = part_ref[far, core] + sib_ref[far]

    totals_arrive()
    weight_total = totals_ref[0] * jnp.exp2(peaks_ref[0] - top)
    for k in range(1, panel_count):
        weight_total = weight_total + totals_ref[k] * jnp.exp2(peaks_ref[k] - top)
    sharp_col[...] = lane_copies(2.0 / weight_total)
    offset_col[...] = lane_copies(resid)
    handed[3].wait_recv()
    run_ref[...] = part_ref[3, core] + sib_ref[3]

    hops[0].wait_recv()
    out_ref[2] = out_ref[2] + in_ref[0]
    hops.append(hop(2, second_peer))
    hops[1].wait_recv()
    run_ref[...] = run_ref[...] + in_ref[1]
    hops[2].wait_recv()

    own = pl.ds(pl.multiple_of(me * LANES, LANES), LANES)

    def finish(r, sums):
        rows = pl.ds(pl.multiple_of(r * ROWS, ROWS), ROWS)
        imputed = (run_ref[rows] + in_ref[2, rows]) * sharp_col[rows]
        dosage = jnp.where(
            flags_ref[rows, own] == 1, tallies_ref[rows, own].astype(jnp.float32), imputed
        )
        dosage_ref[rows] = dosage.astype(jnp.bfloat16)
        score, dose, square = sums
        weighted = offset_col[rows] * dosage
        squared = dosage * dosage
        for k in range(0, ROWS, 8):
            score = score + weighted[k : k + 8]
            dose = dose + dosage[k : k + 8]
            square = square + squared[k : k + 8]
        return score, dose, square

    zero = jnp.zeros((8, LANES), jnp.float32)
    sums = lax.fori_loop(0, samples // ROWS, finish, (zero, zero, zero))
    line = lax.broadcasted_iota(jnp.int32, (8, LANES), 0)
    score, dose, square = (jnp.sum(s, axis=0, keepdims=True) for s in sums)
    stats_ref[depth] = jnp.where(
        line == 0, score, jnp.where(line == 1, dose, jnp.where(line == 2, square, resid_square))
    )
    stats_arrive, stats_sent = share_out(
        stats_ref, stat_send, stat_recv, "samp", samp_count, depth
    )
    stats_arrive()
    stats = stats_ref[0]
    for k in range(1, samp_count):
        stats = stats + stats_ref[k]
    all_samples = float(samples * samp_count)
    sigma = stats[3:4] / (all_samples - GROUPS)
    dose_mean = stats[1:2] / all_samples
    spread = stats[2:3] / all_samples - dose_mean * dose_mean
    zscore_ref[...] = stats[0:1] / jnp.sqrt(sigma * all_samples * (spread + 1e-05))

    for sent in (groups_sent, counts_sent, peaks_sent, totals_sent, stats_sent):
        sent()
    for copy in handed + hops:
        copy.wait_send()


def fused_on_device(panel_count, samp_count, tallies, flags, strands, sharp, trait, cohort):
    samples, variants = tallies.shape
    haps = strands.shape[0]
    f32, bf16, i32 = jnp.float32, jnp.bfloat16, jnp.int32
    column = pltpu.VMEM((samples, LANES), f32)
    peers = pltpu.SemaphoreType.DMA((panel_count - 1,))
    levels = pltpu.SemaphoreType.DMA((samp_count - 1,))
    anywhere = pl.BlockSpec(memory_space=pl.ANY)
    local = pl.BlockSpec(memory_space=pltpu.VMEM)
    dosage, zscore = pl.pallas_call(
        functools.partial(fused, panel_count, samp_count),
        out_shape=(
            jax.ShapeDtypeStruct((samples, LANES), bf16),
            jax.ShapeDtypeStruct((1, LANES), f32),
        ),
        in_specs=[anywhere] * 3 + [local] * 3,
        out_specs=(local, local),
        scratch_shapes=[
            pltpu.VMEM((haps, variants), i32),
            pltpu.VMEM((haps, variants), bf16),
            pltpu.VMEM((samples, variants), i32),
            pltpu.VMEM((samples, variants), i32),
            pltpu.VMEM((samples, variants), bf16),
            pltpu.VMEM((haps // HAP_TILE, samples, HAP_TILE), f32),
            pltpu.VMEM((samples, haps), bf16),
            pltpu.VMEM((panel_count, 1, variants), f32),
            pltpu.VMEM((panel_count, 1, samples), f32),
            pltpu.VMEM((panel_count, 1, samples), f32),
            pltpu.VMEM((samp_count, GROUPS, LANES), f32),
            pltpu.VMEM((samp_count, 8, LANES), f32),
            column,
            column,
            column,
            column,
            pltpu.VMEM((4, 2, samples, LANES), f32),
            pltpu.VMEM((4, samples, LANES), f32),
            pltpu.VMEM((3, samples, LANES), f32),
            pltpu.VMEM((3, samples, LANES), f32),
            pltpu.SemaphoreType.DMA((haps // HAP_TILE,)),
            pltpu.SemaphoreType.DMA((2,)),
            peers,
            peers,
            peers,
            peers,
            peers,
            peers,
            levels,
            levels,
            levels,
            levels,
            pltpu.SemaphoreType.DMA((4,)),
            pltpu.SemaphoreType.DMA((4,)),
            pltpu.SemaphoreType.DMA((3,)),
            pltpu.SemaphoreType.DMA((3,)),
        ],
        compiler_params=pltpu.CompilerParams(
            collective_id=0, has_side_effects=True, vmem_limit_bytes=VMEM_BYTES
        ),
        name="impute",
    )(
        tallies,
        flags,
        strands,
        sharp.reshape(1, samples),
        trait.reshape(1, samples),
        cohort.reshape(1, samples),
    )
    return dosage, zscore.reshape(LANES)


def body_for(mesh):
    panel_count, samp_count = mesh.shape["panel"], mesh.shape["samp"]

    def body(tallies, flags, strands, sharp, trait, cohort):
        samples, variants = tallies.shape
        fits = (
            panel_count == 2 * 2 * 2
            and samp_count > 1
            and variants == panel_count * LANES
            and samples % LANES == 0
            and strands.shape[0] % HAP_TILE == 0
        )
        args = (tallies, flags, strands, sharp, trait, cohort)
        if fits:
            return fused_on_device(panel_count, samp_count, *args)
        return on_device(*args)

    return body


def solution(mesh):
    return jax.shard_map(
        body_for(mesh),
        mesh=mesh,
        in_specs=(
            P("samp", None),
            P("samp", None),
            P("panel", None),
            P("samp"),
            P("samp"),
            P("samp"),
        ),
        out_specs=(P("samp", "panel"), P("panel")),
        check_vma=False,
    )
```

```python
import functools

import jax
import jax.numpy as jnp
from jax import lax
from jax.experimental import pallas as pl
from jax.experimental.pallas import tpu as pltpu
from jax.sharding import PartitionSpec as P

GROUPS = 8


log_two = 0.6931471805599453


def on_device(
    called_allele_tallies,
    presence_flags,
    reference_panel_strands,
    softmax_sharpness,
    trait_measurements,
    cohort_membership,
):
    panel_count = lax.axis_size("panel")
    sample_rows, variants = called_allele_tallies.shape
    local_haps = reference_panel_strands.shape[0]
    hap_float = reference_panel_strands.astype(jnp.float32)
    allele_counts = lax.psum(jnp.sum(hap_float, axis=0), "panel")
    allele_freq = allele_counts / float(local_haps * panel_count)
    geno_float = called_allele_tallies.astype(jnp.float32)
    observed_f = presence_flags.astype(jnp.float32)
    demeaned_expected_count = (observed_f * (geno_float - 2.0 * allele_freq[None, :])).astype(
        jnp.bfloat16
    )
    tile_first_entry = jnp.sum(
        demeaned_expected_count.astype(jnp.float32) * allele_freq[None, :], axis=1
    )
    hap_bf = reference_panel_strands.astype(jnp.bfloat16)
    raw_efficient_statistic = lax.dot_general(
        demeaned_expected_count,
        hap_bf,
        (((1,), (1,)), ((), ())),
        preferred_element_type=jnp.float32,
    )
    panel_match_energies = softmax_sharpness[:, None] * (
        raw_efficient_statistic - tile_first_entry[:, None]
    )
    local_steps = jnp.ceil(jnp.max(panel_match_energies, axis=1) / log_two)
    share = variants // panel_count
    first_column = lax.axis_index("panel") * share
    peak_steps = lax.pmax(local_steps, "panel")
    weights = jnp.exp(panel_match_energies - log_two * peak_steps[:, None])
    weight_total = lax.psum(jnp.sum(weights, axis=1), "panel")
    partial_dose = 2.0 * jnp.dot(
        weights.astype(jnp.bfloat16), hap_bf, preferred_element_type=jnp.float32
    )
    own_dose = lax.psum_scatter(partial_dose, "panel", scatter_dimension=1, tiled=True)
    expected_allele_count = own_dose / weight_total[:, None]
    own_geno = lax.dynamic_slice_in_dim(geno_float, first_column, share, 1)
    own_observed = lax.dynamic_slice_in_dim(presence_flags, first_column, share, 1)
    dosage = jnp.where(own_observed == 1, own_geno, expected_allele_count)
    dosage_out = dosage.astype(jnp.bfloat16)
    member = (cohort_membership[:, None] == jnp.arange(GROUPS, dtype=jnp.int32)[None, :]).astype(
        jnp.float32
    )
    group_sum_local = jnp.dot(trait_measurements, member, precision=lax.Precision.HIGHEST)
    group_count_local = jnp.sum(member, axis=0)
    dose_sum_local = jnp.sum(dosage, axis=0)
    dose_square_local = jnp.sum(dosage * dosage, axis=0)
    all_samples = float(sample_rows * lax.axis_size("samp"))
    group_sum, group_count = lax.psum((group_sum_local, group_count_local), "samp")
    group_mean = group_sum / group_count
    resid = trait_measurements - jnp.dot(member, group_mean, precision=lax.Precision.HIGHEST)
    local_score = jnp.dot(resid, dosage, precision=lax.Precision.HIGHEST)
    score_u, dose_sum, dose_square, resid_square = lax.psum(
        (local_score, dose_sum_local, dose_square_local, jnp.sum(resid * resid)), "samp"
    )
    sigma = resid_square / (all_samples - GROUPS)
    dose_mean = dose_sum / all_samples
    spread = dose_square / all_samples - dose_mean * dose_mean
    zscore = score_u / jnp.sqrt(sigma * all_samples * (spread + 1e-05))
    return (dosage_out, zscore)


MESH = pl.DeviceIdType.MESH
LANES = 128
HAP_TILE = 256
ROWS = 32
VMEM_BYTES = 60 * 1024 * 1024


def lane_copies(row):
    blocks = [
        jnp.broadcast_to(row[:, k : k + LANES], (LANES, LANES)).T
        for k in range(0, row.shape[1], LANES)
    ]
    return jnp.concatenate(blocks, axis=0)


def as_row(column):
    blocks = [
        jnp.broadcast_to(column[k : k + LANES], (LANES, LANES)).T[0:1]
        for k in range(0, column.shape[0], LANES)
    ]
    return jnp.concatenate(blocks, axis=1)


def fused(
    panel_count,
    samp_count,
    tallies_hbm,
    flags_hbm,
    strands_hbm,
    sharp_ref,
    trait_ref,
    cohort_ref,
    dosage_ref,
    zscore_ref,
    strands_ref,
    hap_ref,
    tallies_ref,
    flags_ref,
    code_ref,
    centred_ref,
    logits_ref,
    weights_ref,
    counts_ref,
    peaks_ref,
    chip_peak_ref,
    totals_ref,
    groups_ref,
    stats_ref,
    sharp_col,
    offset_col,
    steps_col,
    mine_col,
    first_col,
    run_ref,
    part_ref,
    sib_ref,
    out_ref,
    in_ref,
    strand_sems,
    load_sems,
    count_send,
    count_recv,
    peak_send,
    peak_recv,
    total_send,
    total_recv,
    group_send,
    group_recv,
    stat_send,
    stat_recv,
    sib_send,
    sib_recv,
    hop_send,
    hop_recv,
):
    me = lax.axis_index("panel")
    depth = lax.axis_index("samp")
    samples, variants = tallies_ref.shape
    haps = strands_ref.shape[0]
    pieces = haps // HAP_TILE
    core = me % 2
    x = (me // 2) % 2
    y = me // 4
    sibling = me + 1 - 2 * core
    x_peer = me + 2 - 4 * x
    y_peer = me + 4 - 8 * y
    first_peer = x_peer + core * (y_peer - x_peer)
    second_peer = y_peer + core * (x_peer - y_peer)

    def strand_load(i):
        rows = pl.ds(i * HAP_TILE, HAP_TILE)
        return pltpu.make_async_copy(
            strands_hbm.at[rows], strands_ref.at[rows], strand_sems.at[i]
        )

    for i in range(pieces):
        strand_load(i).start()
    flag_load = pltpu.make_async_copy(flags_hbm, flags_ref, load_sems.at[0])
    tally_load = pltpu.make_async_copy(tallies_hbm, tallies_ref, load_sems.at[1])

    barrier = pltpu.get_barrier_semaphore()
    for d in range(1, panel_count):
        pl.semaphore_signal(
            barrier, inc=1, device_id={"panel": (me + d) % panel_count}, device_id_type=MESH
        )
    for d in range(1, samp_count):
        pl.semaphore_signal(
            barrier, inc=1, device_id={"samp": (depth + d) % samp_count}, device_id_type=MESH
        )

    def share_out(ref, send, recv, axis, count, mine):
        copies = []
        for d in range(1, count):
            copy = pltpu.make_async_remote_copy(
                src_ref=ref.at[mine],
                dst_ref=ref.at[mine],
                send_sem=send.at[d - 1],
                recv_sem=recv.at[d - 1],
                device_id={axis: (mine + d) % count},
                device_id_type=MESH,
            )
            copy.start()
            copies.append(copy)

        def arrive():
            for d in range(1, count):
                slot = (mine + count - d) % count
                pltpu.make_async_remote_copy(
                    src_ref=ref.at[slot],
                    dst_ref=ref.at[slot],
                    send_sem=send.at[d - 1],
                    recv_sem=recv.at[d - 1],
                    device_id={axis: (mine + d) % count},
                    device_id_type=MESH,
                ).wait_recv()

        def sent():
            for copy in copies:
                copy.wait_send()

        return arrive, sent

    def convert_piece(i, acc):
        strand_load(i).wait()

        def convert_rows(r, acc):
            start = pl.multiple_of(i * HAP_TILE + r * ROWS, ROWS)
            strands = strands_ref[pl.ds(start, ROWS)]
            hap_ref[pl.ds(start, ROWS)] = strands.astype(jnp.float32).astype(jnp.bfloat16)
            for k in range(0, ROWS, 8):
                acc = acc + strands[k : k + 8]
            return acc

        return lax.fori_loop(0, HAP_TILE // ROWS, convert_rows, acc)

    early = pieces // 2
    acc = lax.fori_loop(0, early, convert_piece, jnp.zeros((8, variants), jnp.int32))
    flag_load.start()
    tally_load.start()
    acc = lax.fori_loop(early, pieces, convert_piece, acc)
    pl.semaphore_wait(barrier, panel_count + samp_count - 2)
    counts_ref[me] = jnp.sum(acc.astype(jnp.float32), axis=0, keepdims=True)
    counts_arrive, counts_sent = share_out(
        counts_ref, count_send, count_recv, "panel", panel_count, me
    )
    trait = trait_ref[...]
    member = (
        lax.broadcasted_iota(jnp.int32, (GROUPS, samples), 0)
        == jnp.broadcast_to(cohort_ref[...], (GROUPS, samples))
    ).astype(jnp.float32)
    group_sum = jnp.sum(member * trait, axis=1, keepdims=True)
    group_count = jnp.sum(member, axis=1, keepdims=True)
    lane = lax.broadcasted_iota(jnp.int32, (GROUPS, LANES), 1)
    groups_ref[depth] = jnp.where(lane == 0, group_sum, group_count)
    groups_arrive, groups_sent = share_out(
        groups_ref, group_send, group_recv, "samp", samp_count, depth
    )
    sharp_col[...] = lane_copies(sharp_ref[...])

    flag_load.wait()
    tally_load.wait()

    def encode(r, _):
        rows = pl.ds(pl.multiple_of(r * ROWS, ROWS), ROWS)
        code = jnp.where(flags_ref[rows] == 1, tallies_ref[rows], -1)
        code_ref[rows] = code.astype(jnp.float32)
        return 0

    lax.fori_loop(0, samples // ROWS, encode, 0)

    counts_arrive()
    counts = counts_ref[0]
    for k in range(1, panel_count):
        counts = counts + counts_ref[k]
    freq = counts / float(haps * panel_count)

    twice = 2.0 * freq

    def centre(r, _):
        rows = pl.ds(pl.multiple_of(r * ROWS, ROWS), ROWS)
        code = code_ref[rows]
        centred = jnp.where(code >= 0.0, code - twice, 0.0).astype(jnp.bfloat16)
        centred_ref[rows] = centred
        term = centred.astype(jnp.float32) * freq
        offset = term[:, :LANES]
        for k in range(LANES, variants, LANES):
            offset = offset + term[:, k : k + LANES]
        offset_col[rows] = offset
        return 0

    lax.fori_loop(0, samples // ROWS, centre, 0)
    offset_col[...] = jnp.broadcast_to(
        jnp.sum(offset_col[...], axis=1, keepdims=True), offset_col.shape
    )

    run_ref[...] = jnp.full_like(run_ref, -jnp.inf)

    def match(i, _):
        hap = hap_ref[i * HAP_TILE : (i + 1) * HAP_TILE]
        raw = lax.dot_general(
            centred_ref[...], hap, (((1,), (1,)), ((), ())), preferred_element_type=jnp.float32
        )
        sharp = sharp_col[...]
        offset = offset_col[...]
        best = run_ref[...]
        for k in range(0, HAP_TILE, LANES):
            energy = sharp * (raw[:, k : k + LANES] - offset)
            logits_ref[i, :, k : k + LANES] = energy
            best = jnp.maximum(best, energy)
        run_ref[...] = best
        return 0

    for i in range(pieces):
        match(i, 0)
    steps = jnp.ceil(jnp.max(run_ref[...], axis=1, keepdims=True) / log_two)
    steps_col[...] = jnp.broadcast_to(steps, steps_col.shape)
    local_steps = as_row(steps)
    peaks_ref[me] = local_steps
    sibling_peaks = pltpu.make_async_remote_copy(
        src_ref=peaks_ref.at[me],
        dst_ref=chip_peak_ref,
        send_sem=sib_send.at[4],
        recv_sem=sib_recv.at[4],
        device_id={"panel": sibling},
        device_id_type=MESH,
    )
    sibling_peaks.start()
    peaks_arrive, peaks_sent = share_out(
        peaks_ref, peak_send, peak_recv, "panel", panel_count, me
    )

    run_ref[...] = jnp.zeros_like(run_ref)

    def weigh(r, _):
        rows = pl.ds(pl.multiple_of(r * ROWS, ROWS), ROWS)
        shift = log_two * steps_col[rows]
        total = jnp.zeros((ROWS, LANES), jnp.float32)
        for i in range(pieces):
            for k in range(0, HAP_TILE, LANES):
                weight = jnp.exp(logits_ref[i, rows, k : k + LANES] - shift)
                total = total + weight
                first = i * HAP_TILE + k
                weights_ref[rows, first : first + LANES] = weight.astype(jnp.bfloat16)
        run_ref[rows] = total
        return 0

    lax.fori_loop(0, samples // ROWS, weigh, 0)
    totals_ref[me] = as_row(jnp.sum(run_ref[...], axis=1, keepdims=True))
    totals_arrive, totals_sent = share_out(
        totals_ref, total_send, total_recv, "panel", panel_count, me
    )

    def allele_sums(chip):
        columns = pl.ds(pl.multiple_of(chip * 2 * LANES, 2 * LANES), 2 * LANES)
        half = haps // 2
        return jnp.dot(
            weights_ref[:, :half], hap_ref[:half, columns], preferred_element_type=jnp.float32
        ) + jnp.dot(
            weights_ref[:, half:], hap_ref[half:, columns], preferred_element_type=jnp.float32
        )

    def hand_over(i):
        copy = pltpu.make_async_remote_copy(
            src_ref=part_ref.at[i, 1 - core],
            dst_ref=sib_ref.at[i],
            send_sem=sib_send.at[i],
            recv_sem=sib_recv.at[i],
            device_id={"panel": sibling},
            device_id_type=MESH,
        )
        copy.start()
        return copy

    def hop(i, peer):
        copy = pltpu.make_async_remote_copy(
            src_ref=out_ref.at[i],
            dst_ref=in_ref.at[i],
            send_sem=hop_send.at[i],
            recv_sem=hop_recv.at[i],
            device_id={"panel": peer},
            device_id_type=MESH,
        )
        copy.start()
        return copy

    diag_chip = (1 - y) * 2 + 1 - x
    x_chip = y * 2 + 1 - x
    y_chip = (1 - y) * 2 + x
    own_chip = y * 2 + x
    handed = []
    scale = None
    hops = []
    for i, chip in enumerate((diag_chip, x_chip, y_chip, own_chip)):
        part = allele_sums(chip)
        if i == 0:
            sibling_peaks.wait_recv()
            chip_top = jnp.maximum(local_steps, chip_peak_ref[...])
            steps_col[...] = lane_copies(jnp.exp2(local_steps - chip_top))
        scale = steps_col[...]
        part_ref[i, 0] = scale * part[:, :LANES]
        part_ref[i, 1] = scale * part[:, LANES:]
        handed.append(hand_over(i))
        if i == 1:
            handed[0].wait_recv()
            out_ref[0] = part_ref[0, core] + sib_ref[0]
            hops.append(hop(0, first_peer))

    near = 1 + core
    far = 2 - core
    handed[1].wait_recv()
    handed[2].wait_recv()
    out_ref[1] = part_ref[near, core] + sib_ref[near]
    hops.append(hop(1, first_peer))

    peaks_arrive()
    top = peaks_ref[0]
    for k in range(1, panel_count):
        top = jnp.maximum(top, peaks_ref[k])
    first_top = jnp.maximum(peaks_ref[first_peer], peaks_ref[first_peer + 1 - 2 * core])
    mine_col[...] = lane_copies(jnp.exp2(chip_top - top))
    first_col[...] = lane_copies(jnp.exp2(first_top - top))
    totals_arrive()
    weight_total = totals_ref[0] * jnp.exp2(peaks_ref[0] - top)
    for k in range(1, panel_count):
        weight_total = weight_total + totals_ref[k] * jnp.exp2(peaks_ref[k] - top)
    sharp_col[...] = lane_copies(2.0 / weight_total)
    groups_arrive()
    group_all = groups_ref[0]
    for k in range(1, samp_count):
        group_all = group_all + groups_ref[k]
    group_mean = group_all[:, 0:1] / group_all[:, 1:2]
    resid = trait - jnp.sum(member * group_mean, axis=0, keepdims=True)
    resid_square = jnp.sum(resid * resid, axis=1, keepdims=True)
    offset_col[...] = lane_copies(resid)
    handed[3].wait_recv()
    run_ref[...] = mine_col[...] * (part_ref[3, core] + sib_ref[3])
    out_ref[2] = mine_col[...] * (part_ref[far, core] + sib_ref[far])

    hops[0].wait_recv()
    out_ref[2] = out_ref[2] + first_col[...] * in_ref[0]
    hops.append(hop(2, second_peer))
    hops[1].wait_recv()
    run_ref[...] = run_ref[...] + first_col[...] * in_ref[1]
    hops[2].wait_recv()

    own = pl.ds(pl.multiple_of(me * LANES, LANES), LANES)

    def finish(r, sums):
        rows = pl.ds(pl.multiple_of(r * ROWS, ROWS), ROWS)
        imputed = (run_ref[rows] + in_ref[2, rows]) * sharp_col[rows]
        dosage = jnp.where(
            flags_ref[rows, own] == 1, tallies_ref[rows, own].astype(jnp.float32), imputed
        )
        dosage_ref[rows] = dosage.astype(jnp.bfloat16)
        score, dose, square = sums
        weighted = offset_col[rows] * dosage
        squared = dosage * dosage
        for k in range(0, ROWS, 8):
            score = score + weighted[k : k + 8]
            dose = dose + dosage[k : k + 8]
            square = square + squared[k : k + 8]
        return score, dose, square

    zero = jnp.zeros((8, LANES), jnp.float32)
    sums = lax.fori_loop(0, samples // ROWS, finish, (zero, zero, zero))
    line = lax.broadcasted_iota(jnp.int32, (8, LANES), 0)
    score, dose, square = (jnp.sum(s, axis=0, keepdims=True) for s in sums)
    stats_ref[depth] = jnp.where(
        line == 0, score, jnp.where(line == 1, dose, jnp.where(line == 2, square, resid_square))
    )
    stats_arrive, stats_sent = share_out(
        stats_ref, stat_send, stat_recv, "samp", samp_count, depth
    )
    stats_arrive()
    stats = stats_ref[0]
    for k in range(1, samp_count):
        stats = stats + stats_ref[k]
    all_samples = float(samples * samp_count)
    sigma = stats[3:4] / (all_samples - GROUPS)
    dose_mean = stats[1:2] / all_samples
    spread = stats[2:3] / all_samples - dose_mean * dose_mean
    zscore_ref[...] = stats[0:1] / jnp.sqrt(sigma * all_samples * (spread + 1e-05))

    for sent in (groups_sent, counts_sent, peaks_sent, totals_sent, stats_sent):
        sent()
    for copy in [sibling_peaks] + handed + hops:
        copy.wait_send()


def hand_out(dosage_in, zscore_in, dosage_out, zscore_out):
    dosage_out[...] = dosage_in[...]
    zscore_out[...] = zscore_in[...]


def fused_on_device(panel_count, samp_count, tallies, flags, strands, sharp, trait, cohort):
    samples, variants = tallies.shape
    haps = strands.shape[0]
    f32, bf16, i32 = jnp.float32, jnp.bfloat16, jnp.int32
    column = pltpu.VMEM((samples, LANES), f32)
    peers = pltpu.SemaphoreType.DMA((panel_count - 1,))
    levels = pltpu.SemaphoreType.DMA((samp_count - 1,))
    anywhere = pl.BlockSpec(memory_space=pl.ANY)
    local = pl.BlockSpec(memory_space=pltpu.VMEM)
    dosage, zscore = pl.pallas_call(
        functools.partial(fused, panel_count, samp_count),
        out_shape=(
            jax.ShapeDtypeStruct((samples, LANES), bf16),
            jax.ShapeDtypeStruct((1, LANES), f32),
        ),
        in_specs=[anywhere] * 3 + [local] * 3,
        out_specs=(local, local),
        scratch_shapes=[
            pltpu.VMEM((haps, variants), i32),
            pltpu.VMEM((haps, variants), bf16),
            pltpu.VMEM((samples, variants), i32),
            pltpu.VMEM((samples, variants), i32),
            pltpu.VMEM((samples, variants), f32),
            pltpu.VMEM((samples, variants), bf16),
            pltpu.VMEM((haps // HAP_TILE, samples, HAP_TILE), f32),
            pltpu.VMEM((samples, haps), bf16),
            pltpu.VMEM((panel_count, 1, variants), f32),
            pltpu.VMEM((panel_count, 1, samples), f32),
            pltpu.VMEM((1, samples), f32),
            pltpu.VMEM((panel_count, 1, samples), f32),
            pltpu.VMEM((samp_count, GROUPS, LANES), f32),
            pltpu.VMEM((samp_count, 8, LANES), f32),
            column,
            column,
            column,
            column,
            column,
            column,
            pltpu.VMEM((4, 2, samples, LANES), f32),
            pltpu.VMEM((4, samples, LANES), f32),
            pltpu.VMEM((3, samples, LANES), f32),
            pltpu.VMEM((3, samples, LANES), f32),
            pltpu.SemaphoreType.DMA((haps // HAP_TILE,)),
            pltpu.SemaphoreType.DMA((2,)),
            peers,
            peers,
            peers,
            peers,
            peers,
            peers,
            levels,
            levels,
            levels,
            levels,
            pltpu.SemaphoreType.DMA((5,)),
            pltpu.SemaphoreType.DMA((5,)),
            pltpu.SemaphoreType.DMA((3,)),
            pltpu.SemaphoreType.DMA((3,)),
        ],
        compiler_params=pltpu.CompilerParams(
            collective_id=0, has_side_effects=True, vmem_limit_bytes=VMEM_BYTES
        ),
        name="impute",
    )(
        tallies,
        flags,
        strands,
        sharp.reshape(1, samples),
        trait.reshape(1, samples),
        cohort.reshape(1, samples),
    )
    dosage, zscore = pl.pallas_call(
        hand_out,
        out_shape=(
            jax.ShapeDtypeStruct((samples, LANES), bf16),
            jax.ShapeDtypeStruct((1, LANES), f32),
        ),
        in_specs=[local, local],
        out_specs=(local, local),
        name="hand_out",
    )(dosage, zscore)
    return dosage, zscore.reshape(LANES)


def body_for(mesh):
    panel_count, samp_count = mesh.shape["panel"], mesh.shape["samp"]

    def body(tallies, flags, strands, sharp, trait, cohort):
        samples, variants = tallies.shape
        fits = (
            panel_count == 2 * 2 * 2
            and samp_count > 1
            and variants == panel_count * LANES
            and samples % LANES == 0
            and strands.shape[0] % HAP_TILE == 0
        )
        args = (tallies, flags, strands, sharp, trait, cohort)
        if fits:
            return fused_on_device(panel_count, samp_count, *args)
        return on_device(*args)

    return body


def solution(mesh):
    return jax.shard_map(
        body_for(mesh),
        mesh=mesh,
        in_specs=(
            P("samp", None),
            P("samp", None),
            P("panel", None),
            P("samp"),
            P("samp"),
            P("samp"),
        ),
        out_specs=(P("samp", "panel"), P("panel")),
        check_vma=False,
    )
```

```python
import functools

import jax
import jax.numpy as jnp
from jax import lax
from jax.experimental import pallas as pl
from jax.experimental.pallas import tpu as pltpu
from jax.sharding import PartitionSpec as P

GROUPS = 8


log_two = 0.6931471805599453


def on_device(
    called_allele_tallies,
    presence_flags,
    reference_panel_strands,
    softmax_sharpness,
    trait_measurements,
    cohort_membership,
):
    panel_count = lax.axis_size("panel")
    sample_rows, variants = called_allele_tallies.shape
    local_haps = reference_panel_strands.shape[0]
    hap_float = reference_panel_strands.astype(jnp.float32)
    allele_counts = lax.psum(jnp.sum(hap_float, axis=0), "panel")
    allele_freq = allele_counts / float(local_haps * panel_count)
    geno_float = called_allele_tallies.astype(jnp.float32)
    observed_f = presence_flags.astype(jnp.float32)
    demeaned_expected_count = (observed_f * (geno_float - 2.0 * allele_freq[None, :])).astype(
        jnp.bfloat16
    )
    tile_first_entry = jnp.sum(
        demeaned_expected_count.astype(jnp.float32) * allele_freq[None, :], axis=1
    )
    hap_bf = reference_panel_strands.astype(jnp.bfloat16)
    raw_efficient_statistic = lax.dot_general(
        demeaned_expected_count,
        hap_bf,
        (((1,), (1,)), ((), ())),
        preferred_element_type=jnp.float32,
    )
    panel_match_energies = softmax_sharpness[:, None] * (
        raw_efficient_statistic - tile_first_entry[:, None]
    )
    local_steps = jnp.ceil(jnp.max(panel_match_energies, axis=1) / log_two)
    share = variants // panel_count
    first_column = lax.axis_index("panel") * share
    peak_steps = lax.pmax(local_steps, "panel")
    weights = jnp.exp(panel_match_energies - log_two * peak_steps[:, None])
    weight_total = lax.psum(jnp.sum(weights, axis=1), "panel")
    partial_dose = 2.0 * jnp.dot(
        weights.astype(jnp.bfloat16), hap_bf, preferred_element_type=jnp.float32
    )
    own_dose = lax.psum_scatter(partial_dose, "panel", scatter_dimension=1, tiled=True)
    expected_allele_count = own_dose / weight_total[:, None]
    own_geno = lax.dynamic_slice_in_dim(geno_float, first_column, share, 1)
    own_observed = lax.dynamic_slice_in_dim(presence_flags, first_column, share, 1)
    dosage = jnp.where(own_observed == 1, own_geno, expected_allele_count)
    dosage_out = dosage.astype(jnp.bfloat16)
    member = (cohort_membership[:, None] == jnp.arange(GROUPS, dtype=jnp.int32)[None, :]).astype(
        jnp.float32
    )
    group_sum_local = jnp.dot(trait_measurements, member, precision=lax.Precision.HIGHEST)
    group_count_local = jnp.sum(member, axis=0)
    dose_sum_local = jnp.sum(dosage, axis=0)
    dose_square_local = jnp.sum(dosage * dosage, axis=0)
    all_samples = float(sample_rows * lax.axis_size("samp"))
    group_sum, group_count = lax.psum((group_sum_local, group_count_local), "samp")
    group_mean = group_sum / group_count
    resid = trait_measurements - jnp.dot(member, group_mean, precision=lax.Precision.HIGHEST)
    local_score = jnp.dot(resid, dosage, precision=lax.Precision.HIGHEST)
    score_u, dose_sum, dose_square, resid_square = lax.psum(
        (local_score, dose_sum_local, dose_square_local, jnp.sum(resid * resid)), "samp"
    )
    sigma = resid_square / (all_samples - GROUPS)
    dose_mean = dose_sum / all_samples
    spread = dose_square / all_samples - dose_mean * dose_mean
    zscore = score_u / jnp.sqrt(sigma * all_samples * (spread + 1e-05))
    return (dosage_out, zscore)


MESH = pl.DeviceIdType.MESH
LANES = 128
HAP_TILE = 256
ROWS = 32
VMEM_BYTES = 62 * 1024 * 1024


def lane_copies(row):
    blocks = [
        jnp.broadcast_to(row[:, k : k + LANES], (LANES, LANES)).T
        for k in range(0, row.shape[1], LANES)
    ]
    return jnp.concatenate(blocks, axis=0)


def as_row(column):
    blocks = [
        jnp.broadcast_to(column[k : k + LANES], (LANES, LANES)).T[0:1]
        for k in range(0, column.shape[0], LANES)
    ]
    return jnp.concatenate(blocks, axis=1)


def fused(
    panel_count,
    samp_count,
    tallies_hbm,
    flags_hbm,
    strands_hbm,
    sharp_ref,
    trait_ref,
    cohort_ref,
    dosage_ref,
    zscore_ref,
    strands_ref,
    hap_ref,
    tallies_ref,
    flags_ref,
    code_ref,
    centred_ref,
    logits_ref,
    weights_ref,
    counts_ref,
    peaks_ref,
    chip_peak_ref,
    totals_ref,
    groups_ref,
    stats_ref,
    sharp_col,
    offset_col,
    steps_col,
    mine_col,
    first_col,
    run_ref,
    part_ref,
    sib_ref,
    out_ref,
    in_ref,
    strand_sems,
    load_sems,
    count_send,
    count_recv,
    peak_send,
    peak_recv,
    total_send,
    total_recv,
    group_send,
    group_recv,
    stat_send,
    stat_recv,
    sib_send,
    sib_recv,
    hop_send,
    hop_recv,
):
    me = lax.axis_index("panel")
    depth = lax.axis_index("samp")
    samples, variants = tallies_ref.shape
    haps = strands_ref.shape[0]
    pieces = haps // HAP_TILE
    core = me % 2
    x = (me // 2) % 2
    y = me // 4
    sibling = me + 1 - 2 * core
    x_peer = me + 2 - 4 * x
    y_peer = me + 4 - 8 * y
    first_peer = x_peer + core * (y_peer - x_peer)
    second_peer = y_peer + core * (x_peer - y_peer)

    def strand_load(i):
        rows = pl.ds(i * HAP_TILE, HAP_TILE)
        return pltpu.make_async_copy(
            strands_hbm.at[rows], strands_ref.at[rows], strand_sems.at[i]
        )

    for i in range(pieces):
        strand_load(i).start()
    flag_load = pltpu.make_async_copy(flags_hbm, flags_ref, load_sems.at[0])
    tally_load = pltpu.make_async_copy(tallies_hbm, tallies_ref, load_sems.at[1])

    barrier = pltpu.get_barrier_semaphore()
    for d in range(1, panel_count):
        pl.semaphore_signal(
            barrier, inc=1, device_id={"panel": (me + d) % panel_count}, device_id_type=MESH
        )
    for d in range(1, samp_count):
        pl.semaphore_signal(
            barrier, inc=1, device_id={"samp": (depth + d) % samp_count}, device_id_type=MESH
        )

    def share_out(ref, send, recv, axis, count, mine):
        copies = []
        for d in range(1, count):
            copy = pltpu.make_async_remote_copy(
                src_ref=ref.at[mine],
                dst_ref=ref.at[mine],
                send_sem=send.at[d - 1],
                recv_sem=recv.at[d - 1],
                device_id={axis: (mine + d) % count},
                device_id_type=MESH,
            )
            copy.start()
            copies.append(copy)

        def arrive():
            for d in range(1, count):
                slot = (mine + count - d) % count
                pltpu.make_async_remote_copy(
                    src_ref=ref.at[slot],
                    dst_ref=ref.at[slot],
                    send_sem=send.at[d - 1],
                    recv_sem=recv.at[d - 1],
                    device_id={axis: (mine + d) % count},
                    device_id_type=MESH,
                ).wait_recv()

        def sent():
            for copy in copies:
                copy.wait_send()

        return arrive, sent

    def convert_piece(i, acc):
        strand_load(i).wait()

        def convert_rows(r, acc):
            start = pl.multiple_of(i * HAP_TILE + r * ROWS, ROWS)
            strands = strands_ref[pl.ds(start, ROWS)]
            hap_ref[pl.ds(start, ROWS)] = strands.astype(jnp.float32).astype(jnp.bfloat16)
            for k in range(0, ROWS, 8):
                acc = acc + strands[k : k + 8]
            return acc

        return lax.fori_loop(0, HAP_TILE // ROWS, convert_rows, acc)

    early = pieces // 2
    acc = lax.fori_loop(0, early, convert_piece, jnp.zeros((8, variants), jnp.int32))
    flag_load.start()
    tally_load.start()
    acc = lax.fori_loop(early, pieces, convert_piece, acc)
    pl.semaphore_wait(barrier, panel_count + samp_count - 2)
    counts_ref[me] = jnp.sum(acc.astype(jnp.float32), axis=0, keepdims=True)
    counts_arrive, counts_sent = share_out(
        counts_ref, count_send, count_recv, "panel", panel_count, me
    )
    trait = trait_ref[...]
    member = (
        lax.broadcasted_iota(jnp.int32, (GROUPS, samples), 0)
        == jnp.broadcast_to(cohort_ref[...], (GROUPS, samples))
    ).astype(jnp.float32)
    group_sum = jnp.sum(member * trait, axis=1, keepdims=True)
    group_count = jnp.sum(member, axis=1, keepdims=True)
    lane = lax.broadcasted_iota(jnp.int32, (GROUPS, LANES), 1)
    groups_ref[depth] = jnp.where(lane == 0, group_sum, group_count)
    groups_arrive, groups_sent = share_out(
        groups_ref, group_send, group_recv, "samp", samp_count, depth
    )
    sharp_col[...] = lane_copies(sharp_ref[...])

    flag_load.wait()
    tally_load.wait()

    def encode(r, _):
        rows = pl.ds(pl.multiple_of(r * ROWS, ROWS), ROWS)
        code = jnp.where(flags_ref[rows] == 1, tallies_ref[rows], -1)
        code_ref[rows] = code.astype(jnp.float32)
        return 0

    lax.fori_loop(0, samples // ROWS, encode, 0)

    counts_arrive()
    counts = counts_ref[0]
    for k in range(1, panel_count):
        counts = counts + counts_ref[k]
    freq = counts / float(haps * panel_count)

    twice = 2.0 * freq

    def centre(r, _):
        rows = pl.ds(pl.multiple_of(r * ROWS, ROWS), ROWS)
        code = code_ref[rows]
        centred = jnp.where(code >= 0.0, code - twice, 0.0).astype(jnp.bfloat16)
        centred_ref[rows] = centred
        term = centred.astype(jnp.float32) * freq
        offset = term[:, :LANES]
        for k in range(LANES, variants, LANES):
            offset = offset + term[:, k : k + LANES]
        offset_col[rows] = offset
        return 0

    lax.fori_loop(0, samples // ROWS, centre, 0)
    offset_col[...] = jnp.broadcast_to(
        jnp.sum(offset_col[...], axis=1, keepdims=True), offset_col.shape
    )

    run_ref[...] = jnp.full_like(run_ref, -jnp.inf)

    def match(i, _):
        hap = hap_ref[i * HAP_TILE : (i + 1) * HAP_TILE]
        raw = lax.dot_general(
            centred_ref[...], hap, (((1,), (1,)), ((), ())), preferred_element_type=jnp.float32
        )
        sharp = sharp_col[...]
        offset = offset_col[...]
        best = run_ref[...]
        for k in range(0, HAP_TILE, LANES):
            energy = sharp * (raw[:, k : k + LANES] - offset)
            logits_ref[i, :, k : k + LANES] = energy
            best = jnp.maximum(best, energy)
        run_ref[...] = best
        return 0

    for i in range(pieces):
        match(i, 0)
    steps = jnp.ceil(jnp.max(run_ref[...], axis=1, keepdims=True) / log_two)
    steps_col[...] = jnp.broadcast_to(steps, steps_col.shape)
    local_steps = as_row(steps)
    peaks_ref[me] = local_steps
    sibling_peaks = pltpu.make_async_remote_copy(
        src_ref=peaks_ref.at[me],
        dst_ref=chip_peak_ref,
        send_sem=sib_send.at[4],
        recv_sem=sib_recv.at[4],
        device_id={"panel": sibling},
        device_id_type=MESH,
    )
    sibling_peaks.start()
    peaks_arrive, peaks_sent = share_out(
        peaks_ref, peak_send, peak_recv, "panel", panel_count, me
    )

    run_ref[...] = jnp.zeros_like(run_ref)

    def weigh(r, _):
        rows = pl.ds(pl.multiple_of(r * ROWS, ROWS), ROWS)
        shift = log_two * steps_col[rows]
        total = jnp.zeros((ROWS, LANES), jnp.float32)
        for i in range(pieces):
            for k in range(0, HAP_TILE, LANES):
                weight = jnp.exp(logits_ref[i, rows, k : k + LANES] - shift)
                total = total + weight
                first = i * HAP_TILE + k
                weights_ref[rows, first : first + LANES] = weight.astype(jnp.bfloat16)
        run_ref[rows] = total
        return 0

    lax.fori_loop(0, samples // ROWS, weigh, 0)
    totals_ref[me] = as_row(jnp.sum(run_ref[...], axis=1, keepdims=True))
    totals_arrive, totals_sent = share_out(
        totals_ref, total_send, total_recv, "panel", panel_count, me
    )

    def allele_sums(chip):
        columns = pl.ds(pl.multiple_of(chip * 2 * LANES, 2 * LANES), 2 * LANES)
        half = samples // 2
        hap = hap_ref[:, columns]
        return jnp.concatenate(
            [
                jnp.dot(weights_ref[k : k + half], hap, preferred_element_type=jnp.float32)
                for k in (0, half)
            ],
            axis=0,
        )

    def hand_over(i):
        copy = pltpu.make_async_remote_copy(
            src_ref=part_ref.at[i, 1 - core],
            dst_ref=sib_ref.at[i],
            send_sem=sib_send.at[i],
            recv_sem=sib_recv.at[i],
            device_id={"panel": sibling},
            device_id_type=MESH,
        )
        copy.start()
        return copy

    def hop(i, peer):
        copy = pltpu.make_async_remote_copy(
            src_ref=out_ref.at[i],
            dst_ref=in_ref.at[i],
            send_sem=hop_send.at[i],
            recv_sem=hop_recv.at[i],
            device_id={"panel": peer},
            device_id_type=MESH,
        )
        copy.start()
        return copy

    diag_chip = (1 - y) * 2 + 1 - x
    x_chip = y * 2 + 1 - x
    y_chip = (1 - y) * 2 + x
    own_chip = y * 2 + x
    handed = []
    scale = None
    hops = []
    for i, chip in enumerate((diag_chip, x_chip, y_chip, own_chip)):
        part = allele_sums(chip)
        if i == 0:
            sibling_peaks.wait_recv()
            chip_top = jnp.maximum(local_steps, chip_peak_ref[...])
            steps_col[...] = lane_copies(jnp.exp2(local_steps - chip_top))
        scale = steps_col[...]
        part_ref[i, 0] = scale * part[:, :LANES]
        part_ref[i, 1] = scale * part[:, LANES:]
        handed.append(hand_over(i))
        if i == 1:
            handed[0].wait_recv()
            out_ref[0] = part_ref[0, core] + sib_ref[0]
            hops.append(hop(0, first_peer))

    near = 1 + core
    far = 2 - core
    handed[1].wait_recv()
    handed[2].wait_recv()
    out_ref[1] = part_ref[near, core] + sib_ref[near]
    hops.append(hop(1, first_peer))

    peaks_arrive()
    top = peaks_ref[0]
    for k in range(1, panel_count):
        top = jnp.maximum(top, peaks_ref[k])
    first_top = jnp.maximum(peaks_ref[first_peer], peaks_ref[first_peer + 1 - 2 * core])
    mine_col[...] = lane_copies(jnp.exp2(chip_top - top))
    first_col[...] = lane_copies(jnp.exp2(first_top - top))
    totals_arrive()
    weight_total = totals_ref[0] * jnp.exp2(peaks_ref[0] - top)
    for k in range(1, panel_count):
        weight_total = weight_total + totals_ref[k] * jnp.exp2(peaks_ref[k] - top)
    sharp_col[...] = lane_copies(2.0 / weight_total)
    groups_arrive()
    group_all = groups_ref[0]
    for k in range(1, samp_count):
        group_all = group_all + groups_ref[k]
    group_mean = group_all[:, 0:1] / group_all[:, 1:2]
    resid = trait - jnp.sum(member * group_mean, axis=0, keepdims=True)
    resid_square = jnp.sum(resid * resid, axis=1, keepdims=True)
    offset_col[...] = lane_copies(resid)
    handed[3].wait_recv()
    run_ref[...] = mine_col[...] * (part_ref[3, core] + sib_ref[3])
    out_ref[2] = mine_col[...] * (part_ref[far, core] + sib_ref[far])

    hops[0].wait_recv()
    out_ref[2] = out_ref[2] + first_col[...] * in_ref[0]
    hops.append(hop(2, second_peer))
    hops[1].wait_recv()
    run_ref[...] = run_ref[...] + first_col[...] * in_ref[1]
    hops[2].wait_recv()

    own = pl.ds(pl.multiple_of(me * LANES, LANES), LANES)

    def finish(r, sums):
        rows = pl.ds(pl.multiple_of(r * ROWS, ROWS), ROWS)
        imputed = (run_ref[rows] + in_ref[2, rows]) * sharp_col[rows]
        dosage = jnp.where(
            flags_ref[rows, own] == 1, tallies_ref[rows, own].astype(jnp.float32), imputed
        )
        dosage_ref[rows] = dosage.astype(jnp.bfloat16)
        score, dose, square = sums
        weighted = offset_col[rows] * dosage
        squared = dosage * dosage
        for k in range(0, ROWS, 8):
            score = score + weighted[k : k + 8]
            dose = dose + dosage[k : k + 8]
            square = square + squared[k : k + 8]
        return score, dose, square

    zero = jnp.zeros((8, LANES), jnp.float32)
    sums = lax.fori_loop(0, samples // ROWS, finish, (zero, zero, zero))
    line = lax.broadcasted_iota(jnp.int32, (8, LANES), 0)
    score, dose, square = (jnp.sum(s, axis=0, keepdims=True) for s in sums)
    stats_ref[depth] = jnp.where(
        line == 0, score, jnp.where(line == 1, dose, jnp.where(line == 2, square, resid_square))
    )
    stats_arrive, stats_sent = share_out(
        stats_ref, stat_send, stat_recv, "samp", samp_count, depth
    )
    stats_arrive()
    stats = stats_ref[0]
    for k in range(1, samp_count):
        stats = stats + stats_ref[k]
    all_samples = float(samples * samp_count)
    sigma = stats[3:4] / (all_samples - GROUPS)
    dose_mean = stats[1:2] / all_samples
    spread = stats[2:3] / all_samples - dose_mean * dose_mean
    zscore_ref[...] = stats[0:1] / jnp.sqrt(sigma * all_samples * (spread + 1e-05))

    for sent in (groups_sent, counts_sent, peaks_sent, totals_sent, stats_sent):
        sent()
    for copy in [sibling_peaks] + handed + hops:
        copy.wait_send()


def fused_on_device(panel_count, samp_count, tallies, flags, strands, sharp, trait, cohort):
    samples, variants = tallies.shape
    haps = strands.shape[0]
    f32, bf16, i32 = jnp.float32, jnp.bfloat16, jnp.int32
    column = pltpu.VMEM((samples, LANES), f32)
    peers = pltpu.SemaphoreType.DMA((panel_count - 1,))
    levels = pltpu.SemaphoreType.DMA((samp_count - 1,))
    anywhere = pl.BlockSpec(memory_space=pl.ANY)
    local = pl.BlockSpec(memory_space=pltpu.VMEM)
    dosage, zscore = pl.pallas_call(
        functools.partial(fused, panel_count, samp_count),
        out_shape=(
            pltpu.VMEM((samples, LANES), bf16),
            pltpu.VMEM((1, LANES), f32),
        ),
        in_specs=[anywhere] * 3 + [local] * 3,
        out_specs=(local, local),
        scratch_shapes=[
            pltpu.VMEM((haps, variants), i32),
            pltpu.VMEM((haps, variants), bf16),
            pltpu.VMEM((samples, variants), i32),
            pltpu.VMEM((samples, variants), i32),
            pltpu.VMEM((samples, variants), f32),
            pltpu.VMEM((samples, variants), bf16),
            pltpu.VMEM((haps // HAP_TILE, samples, HAP_TILE), f32),
            pltpu.VMEM((samples, haps), bf16),
            pltpu.VMEM((panel_count, 1, variants), f32),
            pltpu.VMEM((panel_count, 1, samples), f32),
            pltpu.VMEM((1, samples), f32),
            pltpu.VMEM((panel_count, 1, samples), f32),
            pltpu.VMEM((samp_count, GROUPS, LANES), f32),
            pltpu.VMEM((samp_count, 8, LANES), f32),
            column,
            column,
            column,
            column,
            column,
            column,
            pltpu.VMEM((4, 2, samples, LANES), f32),
            pltpu.VMEM((4, samples, LANES), f32),
            pltpu.VMEM((3, samples, LANES), f32),
            pltpu.VMEM((3, samples, LANES), f32),
            pltpu.SemaphoreType.DMA((haps // HAP_TILE,)),
            pltpu.SemaphoreType.DMA((2,)),
            peers,
            peers,
            peers,
            peers,
            peers,
            peers,
            levels,
            levels,
            levels,
            levels,
            pltpu.SemaphoreType.DMA((5,)),
            pltpu.SemaphoreType.DMA((5,)),
            pltpu.SemaphoreType.DMA((3,)),
            pltpu.SemaphoreType.DMA((3,)),
        ],
        compiler_params=pltpu.CompilerParams(
            collective_id=0, has_side_effects=True, vmem_limit_bytes=VMEM_BYTES
        ),
        name="impute",
    )(
        tallies,
        flags,
        strands,
        sharp.reshape(1, samples),
        trait.reshape(1, samples),
        cohort.reshape(1, samples),
    )
    return dosage, zscore.reshape(LANES)


def body_for(mesh):
    panel_count, samp_count = mesh.shape["panel"], mesh.shape["samp"]

    def body(tallies, flags, strands, sharp, trait, cohort):
        samples, variants = tallies.shape
        fits = (
            panel_count == 2 * 2 * 2
            and samp_count > 1
            and variants == panel_count * LANES
            and samples % LANES == 0
            and strands.shape[0] % HAP_TILE == 0
        )
        args = (tallies, flags, strands, sharp, trait, cohort)
        if fits:
            return fused_on_device(panel_count, samp_count, *args)
        return on_device(*args)

    return body


def solution(mesh):
    return jax.shard_map(
        body_for(mesh),
        mesh=mesh,
        in_specs=(
            P("samp", None),
            P("samp", None),
            P("panel", None),
            P("samp"),
            P("samp"),
            P("samp"),
        ),
        out_specs=(P("samp", "panel"), P("panel")),
        check_vma=False,
    )
```
